32 devices in a mesh: prow: 8 (over z, x), pcol: 4 (over y, core).
Axes of the slice: x: 2, y: 2, z: 4, core: 2. Of those that a mesh axis runs over, the one named last changes fastest.
Arguments:
- matrix: float32 [16384, 16384], P('prow', 'pcol'), may hold values from -6 to 6
Outputs:
- reduced: float32 [16384, 16384], P('prow', 'pcol')
- householder_coefficients: float32 [2, 8], replicated
The draws below stay inside these ranges and needn't reach their ends.
All inputs are finite; a program needn't handle non-finite values.
Results may differ from the reference program's by a relative error of at most 0.0003.
Values sent between devices are 32-bit elements; how exact they have to be, the bound alone decides.
A program may use at most 128 MiB of HBM per device.

```python
import jax
import jax.numpy as jnp
from jax import lax

N = 16384
NB = 8
WINDOWS = 1


def block_scale(stream_key, shape, shards, low, high):
    loudness, own = 1.0, jax.random.fold_in(stream_key, 6)
    for dim, shards_of in shards:
        steps = jnp.exp(jax.random.uniform(jax.random.fold_in(own, dim), (shards_of,), jnp.float32, low / len(shards), high / len(shards)))
        loudness = loudness * jnp.repeat(steps, shape[dim] // shards_of).reshape([-1 if axis == dim else 1 for axis in range(len(shape))])
    return loudness


def normal_values(key, shape, spread, most, shards=(), kind=jnp.bfloat16):
    level = block_scale(key, shape, shards, -0.22, 0.18) if shards else 1.0
    values = jax.random.normal(key, shape, jnp.float32) * spread * level
    return jnp.minimum(jnp.maximum(values, -most), most).astype(kind)


def setup_inputs(seed: int = 0) -> dict:
    streams_of = jax.random.split(jax.random.key(seed), 2)
    matrix = normal_values(streams_of[0], (N, N), 1.0, 6.0, ((0, 8), (1, 4)), jnp.float32)
    return {"matrix": matrix}


epsilon = 1e-06

def precise_dot(left, right):
    return jnp.dot(left, right, precision=lax.Precision.HIGHEST)

def householder(alpha_value, sumsq):
    norm_value = jnp.sqrt(sumsq + epsilon)
    signum = jnp.where(alpha_value >= 0.0, 1.0, -1.0).astype(jnp.float32)
    beta_value = -signum * norm_value
    return (beta_value, (beta_value - alpha_value) / beta_value, alpha_value - beta_value)

def reference(matrix):
    row_index = jnp.arange(N, dtype=jnp.int32)
    col_index = jnp.arange(N, dtype=jnp.int32)
    panel_index = jnp.arange(NB, dtype=jnp.int32)
    working_array = matrix
    source_side_factor_list = []
    target_side_factor_list = []
    for window in range(WINDOWS):
        offset = window * NB
        v_rows = jnp.zeros((NB, N), jnp.float32)
        x_rows = jnp.zeros((NB, N), jnp.float32)
        y_cols = jnp.zeros((NB, N), jnp.float32)
        u_cols = jnp.zeros((NB, N), jnp.float32)
        diagonal_entries = []
        super_list = []
        for i in range(NB):
            k = offset + i
            column = working_array[:, k] - precise_dot(y_cols[:, k], v_rows) - precise_dot(u_cols[:, k], x_rows)
            masked = jnp.where(row_index >= k, column, 0.0)
            beta_left, source_side_coefficient, denom_left = householder(column[k], jnp.sum(masked * masked))
            v_new = (masked - beta_left * (row_index == k).astype(jnp.float32)) / denom_left
            transposed = precise_dot(v_new, working_array) - precise_dot(precise_dot(v_rows, v_new), y_cols) - precise_dot(precise_dot(x_rows, v_new), u_cols)
            y_new = jnp.where(col_index > k, source_side_coefficient * transposed, 0.0)
            v_rows = v_rows.at[i].set(v_new)
            y_cols = y_cols.at[i].set(y_new)
            row_eff = working_array[k, :] - precise_dot(v_rows[:, k], y_cols) - precise_dot(x_rows[:, k], u_cols)
            row_masked = jnp.where(col_index >= k + 1, row_eff, 0.0)
            right_reflector_beta, target_side_coefficient, denom_right = householder(row_eff[k + 1], jnp.sum(row_masked * row_masked))
            u_new = (row_masked - right_reflector_beta * (col_index == k + 1).astype(jnp.float32)) / denom_right
            product = precise_dot(working_array, u_new) - precise_dot(precise_dot(y_cols, u_new), v_rows) - precise_dot(precise_dot(u_cols, u_new), x_rows)
            x_new = jnp.where(row_index > k, target_side_coefficient * product, 0.0)
            x_rows = x_rows.at[i].set(x_new)
            u_cols = u_cols.at[i].set(u_new)
            diagonal_entries.append(beta_left)
            super_list.append(right_reflector_beta)
            source_side_factor_list.append(source_side_coefficient)
            target_side_factor_list.append(target_side_coefficient)
        stack_left = jnp.concatenate([v_rows, x_rows], axis=0)
        stack_right = jnp.concatenate([y_cols, u_cols], axis=0)
        updated = working_array - lax.dot_general(stack_left, stack_right, (((0,), (0,)), ((), ())), precision=lax.Precision.HIGHEST)
        updated = updated.at[offset + NB:, offset:offset + NB].set(v_rows[:, offset + NB:].T)
        row_glob = (offset + panel_index)[:, None]
        col_g = col_index[None, :]
        v_window = jnp.where(panel_index[None, :] < panel_index[:, None], v_rows[:, offset:offset + NB].T, 0.0)
        v_part = jnp.zeros((NB, N), jnp.float32).at[:, offset:offset + NB].set(v_window)
        diag_arr = jnp.stack(diagonal_entries)[:, None]
        super_arr = jnp.stack(super_list)[:, None]
        panel_values = jnp.where(col_g < offset, updated[offset:offset + NB, :], jnp.where(col_g < row_glob, v_part, jnp.where(col_g == row_glob, diag_arr, jnp.where(col_g == row_glob + 1, super_arr, u_cols))))
        working_array = updated.at[offset:offset + NB, :].set(panel_values)
    householder_coefficients = jnp.stack([jnp.stack(source_side_factor_list), jnp.stack(target_side_factor_list)])
    return (working_array, householder_coefficients)
```

```python
import functools

import jax
import jax.numpy as jnp
from jax import lax
from jax.experimental import pallas as pl
from jax.experimental.pallas import tpu as pltpu
from jax.sharding import PartitionSpec as P

NB = 8
EPS = 1e-06
LANES = 128
YC = 4
XC = 2
MESH = pl.DeviceIdType.MESH


def householder(alpha, sumsq):
    beta = jnp.where(alpha >= 0.0, -1.0, 1.0) * jnp.sqrt(sumsq + EPS)
    return beta, (beta - alpha) / beta, alpha - beta


def lane_sum(x):
    return jnp.sum(x, axis=1, keepdims=True)


def total(x):
    return jnp.sum(lane_sum(x), axis=0, keepdims=True)


def panel_kernel(np_, nq, a_hbm, left_o, right_o, scal_o,
                 a, strip, arows, colp, rowp, v_s, x_s, y_s, u_s, vb, ub,
                 ybuf, xbuf, column_s,
                 a_sem, strip_sem, arow_sem, col_ssem, col_rsem, row_ssem, row_rsem,
                 y_ssem, y_rsem, x_ssem, x_rsem):
    me_p = lax.axis_index("prow")
    me_q = lax.axis_index("pcol")
    rows, cols = a.shape
    rs, cs = rows // LANES, cols // LANES
    chunk = cols // YC
    per = chunk // LANES
    xper = rs // XC

    strip_cp = pltpu.make_async_copy(a_hbm.at[:, pl.ds(0, LANES)], strip, strip_sem)
    strip_cp.start()
    arow_cp = pltpu.make_async_copy(a_hbm.at[pl.ds(0, NB), :], arows, arow_sem)
    arow_cp.start()
    a_cps = []
    for c in range(YC):
        cp = pltpu.make_async_copy(
            a_hbm.at[:, pl.ds(c * chunk, chunk)], a.at[:, pl.ds(c * chunk, chunk)], a_sem.at[c])
        cp.start()
        a_cps.append(cp)

    barrier = pltpu.get_barrier_semaphore()
    for d in range(1, np_):
        pl.semaphore_signal(barrier, inc=1, device_id={"prow": lax.rem(me_p + d, np_)}, device_id_type=MESH)
    for d in range(1, nq):
        pl.semaphore_signal(barrier, inc=1, device_id={"pcol": lax.rem(me_q + d, nq)}, device_id_type=MESH)
    pl.semaphore_wait(barrier, np_ + nq - 2)

    lane8 = lax.broadcasted_iota(jnp.int32, (8, LANES), 1)
    sub8 = lax.broadcasted_iota(jnp.int32, (8, LANES), 0)
    row_gl = (me_p * rows + lax.broadcasted_iota(jnp.int32, (rs, LANES), 0) * LANES
              + lax.broadcasted_iota(jnp.int32, (rs, LANES), 1))
    col_gl = (me_q * cols + lax.broadcasted_iota(jnp.int32, (cs, LANES), 0) * LANES
              + lax.broadcasted_iota(jnp.int32, (cs, LANES), 1))

    strip_cp.wait()
    arow_cp.wait()

    def col_copy(d):
        return pltpu.make_async_remote_copy(
            src_ref=colp, dst_ref=colp, send_sem=col_ssem.at[d], recv_sem=col_rsem,
            device_id={"pcol": lax.rem(me_q + d, nq)}, device_id_type=MESH)

    def row_copy(i, d):
        return pltpu.make_async_remote_copy(
            src_ref=rowp.at[i], dst_ref=rowp.at[i], send_sem=row_ssem.at[i, d], recv_sem=row_rsem.at[i],
            device_id={"prow": lax.rem(me_p + d, np_)}, device_id_type=MESH)

    @pl.when(me_q == 0)
    def _():
        @pl.loop(0, rs)
        def _(s):
            t = strip[pl.ds(s * LANES, LANES), :].T
            for c in range(NB + 1):
                colp[c, pl.ds(s, 1), :] = t[c:c + 1, :]
        for d in range(1, nq):
            col_copy(d).start()

    @pl.when(me_p == 0)
    def _():
        for s in range(cs):
            blk = arows[:, s * LANES:(s + 1) * LANES]
            for i in range(NB):
                rowp[i, s:s + 1, :] = blk[i:i + 1, :]
        for i in range(2):
            for d in range(1, np_):
                row_copy(i, d).start()

    for ref in (v_s, x_s, y_s, u_s):
        ref[...] = jnp.zeros(ref.shape, jnp.float32)

    @pl.when(me_q != 0)
    def _():
        col_copy(1).wait_recv()

    column_s[...] = colp[0]

    def y_copy(i, d, c):
        lo, n = (0, 8 + per) if c == 0 else (8 + c * per, per)
        ref = ybuf.at[i, me_p, pl.ds(lo, n), :]
        return pltpu.make_async_remote_copy(
            src_ref=ref, dst_ref=ref, send_sem=y_ssem.at[d, c], recv_sem=y_rsem.at[lax.rem(i, 2), d, c],
            device_id={"prow": lax.rem(me_p + d, np_)}, device_id_type=MESH)

    def x_copy(i, d, c):
        lo, n = (0, 8 + xper) if c == 0 else (8 + c * xper, xper)
        ref = xbuf.at[i, me_q, pl.ds(lo, n), :]
        return pltpu.make_async_remote_copy(
            src_ref=ref, dst_ref=ref, send_sem=x_ssem.at[d, c], recv_sem=x_rsem.at[lax.rem(i, 2), d, c],
            device_id={"pcol": lax.rem(me_q + d, nq)}, device_id_type=MESH)

    def scalar_tile(first, second, vec, unit):
        tile = jnp.zeros((8, LANES), jnp.float32)
        for k, (ref, w) in enumerate(((first, vec), (second, vec), (first, unit), (second, unit))):
            s = lane_sum(jnp.sum(ref[...] * w[None], axis=1))
            tile = jnp.where(lane8 == k, s, tile)
        s = jnp.where(sub8[:, :1] == 0, total(vec * unit), total(vec * vec))
        return jnp.where(lane8 == 4, s, tile)

    def unpack(tile):
        return [jnp.broadcast_to(lane_sum(jnp.where(lane8 == k, tile, 0.0)), (8, LANES)) for k in range(5)]

    def combine(coef_a, ref_a, coef_b, ref_b):
        acc = coef_a[0:1] * ref_a[0] + coef_b[0:1] * ref_b[0]
        for j in range(1, NB):
            acc = acc + (coef_a[j:j + 1] * ref_a[j] + coef_b[j:j + 1] * ref_b[j])
        return acc

    @pl.loop(0, NB)
    def _(i):
        masked = jnp.where(row_gl >= i, column_s[...], 0.0)
        unit_r = (row_gl == i).astype(jnp.float32)
        column_s[...] = masked

        @pl.loop(0, rs)
        def _(s):
            row = jnp.broadcast_to(column_s[pl.ds(s, 1), :], (8, LANES))
            for g in range(LANES // 8):
                col = lane_sum(jnp.where(lane8 == sub8 + 8 * g, row, 0.0))
                vb[pl.ds(s * LANES + 8 * g, 8), :] = jnp.broadcast_to(col, (8, LANES))

        ybuf[i, me_p, 0:8, :] = scalar_tile(v_s, x_s, masked, unit_r)
        for c in range(YC):
            @pl.when(i == 0)
            def _(c=c):
                a_cps[c].wait()

            def body(g, accs):
                accs = list(accs)
                for k in range(8):
                    r = pl.ds(pl.multiple_of(g * 64 + 8 * k, 8), 8)
                    v = vb[r, :]
                    for j in range(per):
                        lo = c * chunk + j * LANES
                        m = (k % 2) * per + j
                        accs[m] = accs[m] + v * a[r, lo:lo + LANES]
                return tuple(accs)

            accs = lax.fori_loop(0, rows // 64, body, (jnp.zeros((8, LANES), jnp.float32),) * (2 * per))
            for j in range(per):
                t = 8 + c * per + j
                ybuf[i, me_p, t:t + 1, :] = jnp.sum(accs[j] + accs[per + j], axis=0, keepdims=True)
            for d in range(1, np_):
                y_copy(i, d, c).start()

        @pl.when(jnp.logical_and(me_p == 0, i < NB - 2))
        def _():
            for d in range(1, np_):
                row_copy(i + 2, d).start()

        @pl.when(me_p != 0)
        def _():
            row_copy(i, 1).wait_recv()

        for c in range(YC):
            for d in range(1, np_):
                y_copy(i, d, c).wait()
        summed = ybuf[i, 0]
        for p in range(1, np_):
            summed = summed + ybuf[i, p]
        v_coef, x_coef, v_at, x_at, misc = unpack(summed[0:8])
        beta, tau, denom = householder(misc[0:1], misc[1:2])
        row_eff = rowp[i] - combine(v_at, y_s, x_at, u_s)
        inv = 1.0 / denom
        trans = (summed[8:] - combine(v_coef, y_s, x_coef, u_s) - beta * row_eff) * inv
        y_new = jnp.where(col_gl > i, tau * trans, 0.0)
        v_s[i] = (masked - beta * unit_r) * inv
        y_s[i] = y_new
        scal_o[0, pl.ds(i, 1), :] = beta
        scal_o[2, pl.ds(i, 1), :] = tau

        row_m = jnp.where(col_gl > i, row_eff - y_new, 0.0)
        unit_c = (col_gl == i + 1).astype(jnp.float32)
        ub[...] = row_m
        xbuf[i, me_q, 0:8, :] = scalar_tile(y_s, u_s, row_m, unit_c)
        for c in range(XC):
            @pl.loop(c * xper, (c + 1) * xper)
            def _(s):
                us = [jnp.broadcast_to(ub[j:j + 1, :], (8, LANES)) for j in range(cs)]
                tile = jnp.zeros((8, LANES), jnp.float32)
                for g in range(LANES // 8):
                    r = pl.ds(pl.multiple_of(s * LANES + 8 * g, 8), 8)
                    p0 = us[0] * a[r, 0:LANES]
                    p1 = us[1] * a[r, LANES:2 * LANES]
                    for j in range(2, cs, 2):
                        p0 = p0 + us[j] * a[r, j * LANES:(j + 1) * LANES]
                        p1 = p1 + us[j + 1] * a[r, (j + 1) * LANES:(j + 2) * LANES]
                    tile = jnp.where(lane8 == sub8 + 8 * g, lane_sum(p0 + p1), tile)
                xbuf[i, me_q, pl.ds(8 + s, 1), :] = jnp.sum(tile, axis=0, keepdims=True)
            for d in range(1, nq):
                x_copy(i, d, c).start()
        for c in range(XC):
            for d in range(1, nq):
                x_copy(i, d, c).wait()
        xsum = xbuf[i, 0]
        for q in range(1, nq):
            xsum = xsum + xbuf[i, q]
        y_coef, u_coef, y_at, u_at, misc2 = unpack(xsum[0:8])
        beta2, tau2, denom2 = householder(misc2[0:1], misc2[1:2])
        col_next = colp[i + 1] - combine(y_at, v_s, u_at, x_s)
        inv2 = 1.0 / denom2
        prod = (xsum[8:] - combine(y_coef, v_s, u_coef, x_s) - beta2 * col_next) * inv2
        x_new = jnp.where(row_gl > i, tau2 * prod, 0.0)
        x_s[i] = x_new
        u_s[i] = (row_m - beta2 * unit_c) * inv2
        scal_o[1, pl.ds(i, 1), :] = beta2
        scal_o[3, pl.ds(i, 1), :] = tau2
        column_s[...] = col_next - x_new

    for s in range(rs):
        left_o[0:NB, s * LANES:(s + 1) * LANES] = v_s[:, s, :]
        left_o[NB:, s * LANES:(s + 1) * LANES] = x_s[:, s, :]
    for s in range(cs):
        right_o[0:NB, s * LANES:(s + 1) * LANES] = y_s[:, s, :]
        right_o[NB:, s * LANES:(s + 1) * LANES] = u_s[:, s, :]

    @pl.when(me_q == 0)
    def _():
        for d in range(1, nq):
            col_copy(d).wait_send()

    @pl.when(me_p == 0)
    def _():
        @pl.loop(0, NB)
        def _(i):
            for d in range(1, np_):
                row_copy(i, d).wait_send()


def reduce_panel(matrix, np_, nq):
    rows, cols = matrix.shape
    rs, cs = rows // LANES, cols // LANES
    f32 = jnp.float32
    vmem = pl.BlockSpec(memory_space=pltpu.VMEM)
    dma = pltpu.SemaphoreType.DMA
    return pl.pallas_call(
        functools.partial(panel_kernel, np_, nq),
        out_shape=(jax.ShapeDtypeStruct((2 * NB, rows), f32),
                   jax.ShapeDtypeStruct((2 * NB, cols), f32),
                   jax.ShapeDtypeStruct((4, NB, LANES), f32)),
        in_specs=[pl.BlockSpec(memory_space=pl.ANY)],
        out_specs=(vmem, vmem, vmem),
        scratch_shapes=[
            pltpu.VMEM((rows, cols), f32),
            pltpu.VMEM((rows, LANES), f32),
            pltpu.VMEM((NB, cols), f32),
            pltpu.VMEM((NB + 1, rs, LANES), f32),
            pltpu.VMEM((NB, cs, LANES), f32),
            pltpu.VMEM((NB, rs, LANES), f32),
            pltpu.VMEM((NB, rs, LANES), f32),
            pltpu.VMEM((NB, cs, LANES), f32),
            pltpu.VMEM((NB, cs, LANES), f32),
            pltpu.VMEM((rows, LANES), f32),
            pltpu.VMEM((cs, LANES), f32),
            pltpu.VMEM((NB, np_, 8 + cs, LANES), f32),
            pltpu.VMEM((NB, nq, 8 + rs, LANES), f32),
            pltpu.VMEM((rs, LANES), f32),
            dma((YC,)), dma, dma,
            dma((nq,)), dma, dma((NB, np_)), dma((NB,)),
            dma((np_, YC)), dma((2, np_, YC)), dma((nq, XC)), dma((2, nq, XC)),
        ],
        compiler_params=pltpu.CompilerParams(
            collective_id=0, has_side_effects=True, vmem_limit_bytes=60 * 1024 * 1024),
    )(matrix)


def pieces(x):
    hi = x.astype(jnp.bfloat16)
    rest = x - hi.astype(jnp.float32)
    mid = rest.astype(jnp.bfloat16)
    lo = (rest - mid.astype(jnp.float32)).astype(jnp.bfloat16)
    return hi, mid, lo


def update_kernel(a_ref, left_ref, right_ref, scal_ref, out_ref):
    me_p = lax.axis_index("prow")
    me_q = lax.axis_index("pcol")
    step = pl.program_id(0)
    block, cols = a_ref.shape
    lh, lm, ll = pieces(left_ref[...])
    rh, rm, rl = pieces(right_ref[...])
    left = jnp.concatenate([lh, lh, lh, lm, lm, ll], axis=0)
    right = jnp.concatenate([rh, rm, rl, rh, rm, rh], axis=0)
    dims = (((0,), (0,)), ((), ()))
    out_ref[...] = a_ref[...] - lax.dot_general(left, right, dims, preferred_element_type=jnp.float32)

    k = left.shape[0]
    src = lax.broadcasted_iota(jnp.int32, (k, LANES), 0)
    lane = lax.broadcasted_iota(jnp.int32, (k, LANES), 1)
    pick = jnp.logical_and(
        lane < NB, (src == lane) | (src == lane + 6 * NB) | (src == lane + 10 * NB))
    vt = lax.dot_general(left, jnp.where(pick, 1.0, 0.0).astype(jnp.bfloat16), dims,
                         preferred_element_type=jnp.float32)

    @pl.when(me_q == 0)
    def _():
        lanes = lax.broadcasted_iota(jnp.int32, (block, LANES), 1)
        out_ref[:, 0:LANES] = jnp.where(lanes < NB, vt, out_ref[:, 0:LANES])

    @pl.when(jnp.logical_and(me_p == 0, step == 0))
    def _():
        out_ref[0:NB, :] = right_ref[NB:, :]

        @pl.when(me_q == 0)
        def _():
            r = lax.broadcasted_iota(jnp.int32, (NB, LANES), 0)
            c = lax.broadcasted_iota(jnp.int32, (NB, LANES), 1)
            out_ref[0:NB, 0:LANES] = jnp.where(
                c < r, vt[0:NB, :],
                jnp.where(c == r, scal_ref[0], jnp.where(c == r + 1, scal_ref[1], right_ref[NB:, 0:LANES])))


def apply_panel(matrix, left, right, scal):
    rows, cols = matrix.shape
    block = min(rows, 256)
    return pl.pallas_call(
        update_kernel,
        out_shape=jax.ShapeDtypeStruct((rows, cols), jnp.float32),
        grid=(rows // block,),
        in_specs=[
            pl.BlockSpec((block, cols), lambda i: (i, 0)),
            pl.BlockSpec((2 * NB, block), lambda i: (0, i)),
            pl.BlockSpec((2 * NB, cols), lambda i: (0, 0)),
            pl.BlockSpec((4, NB, LANES), lambda i: (0, 0, 0)),
        ],
        out_specs=pl.BlockSpec((block, cols), lambda i: (i, 0)),
        compiler_params=pltpu.CompilerParams(vmem_limit_bytes=48 * 1024 * 1024),
    )(matrix, left, right, scal)


def solution(mesh):
    np_, nq = mesh.shape["prow"], mesh.shape["pcol"]

    def per_device(matrix):
        left, right, scal = reduce_panel(matrix, np_, nq)
        return apply_panel(matrix, left, right, scal), scal[2:4, :, 0]

    return jax.shard_map(
        per_device, mesh=mesh, in_specs=(P("prow", "pcol"),),
        out_specs=(P("prow", "pcol"), P()), check_vma=False)
```

```python
import functools

import jax
import jax.numpy as jnp
from jax import lax
from jax.experimental import pallas as pl
from jax.experimental.pallas import tpu as pltpu
from jax.sharding import PartitionSpec as P

NB = 8
EPS = 1e-06
LANES = 128
YC = 4
XC = 2
MESH = pl.DeviceIdType.MESH


def householder(alpha, sumsq):
    beta = jnp.where(alpha >= 0.0, -1.0, 1.0) * jnp.sqrt(sumsq + EPS)
    return beta, (beta - alpha) / beta, alpha - beta


def lane_sum(x):
    return jnp.sum(x, axis=1, keepdims=True)


def total(x):
    return jnp.sum(lane_sum(x), axis=0, keepdims=True)


def panel_kernel(np_, nq, a_hbm, left_o, right_o, scal_o,
                 a, strip, arows, colp, rowp, v_s, x_s, y_s, u_s, vb, ub,
                 ybuf, xbuf, column_s,
                 a_sem, strip_sem, arow_sem, col_ssem, col_rsem, row_ssem, row_rsem,
                 y_ssem, y_rsem, x_ssem, x_rsem):
    me_p = lax.axis_index("prow")
    me_q = lax.axis_index("pcol")
    rows, cols = a.shape
    rs, cs = rows // LANES, cols // LANES
    chunk = cols // YC
    per = chunk // LANES
    xper = rs // XC

    strip_cp = pltpu.make_async_copy(a_hbm.at[:, pl.ds(0, LANES)], strip, strip_sem)
    strip_cp.start()
    arow_cp = pltpu.make_async_copy(a_hbm.at[pl.ds(0, NB), :], arows, arow_sem)
    arow_cp.start()
    a_cps = []
    for c in range(YC):
        cp = pltpu.make_async_copy(
            a_hbm.at[:, pl.ds(c * chunk, chunk)], a.at[:, pl.ds(c * chunk, chunk)], a_sem.at[c])
        cp.start()
        a_cps.append(cp)

    barrier = pltpu.get_barrier_semaphore()
    for d in range(1, np_):
        pl.semaphore_signal(barrier, inc=1, device_id={"prow": lax.rem(me_p + d, np_)}, device_id_type=MESH)
    for d in range(1, nq):
        pl.semaphore_signal(barrier, inc=1, device_id={"pcol": lax.rem(me_q + d, nq)}, device_id_type=MESH)
    pl.semaphore_wait(barrier, np_ + nq - 2)

    lane8 = lax.broadcasted_iota(jnp.int32, (8, LANES), 1)
    sub8 = lax.broadcasted_iota(jnp.int32, (8, LANES), 0)
    row_gl = (me_p * rows + lax.broadcasted_iota(jnp.int32, (rs, LANES), 0) * LANES
              + lax.broadcasted_iota(jnp.int32, (rs, LANES), 1))
    col_gl = (me_q * cols + lax.broadcasted_iota(jnp.int32, (cs, LANES), 0) * LANES
              + lax.broadcasted_iota(jnp.int32, (cs, LANES), 1))

    strip_cp.wait()
    arow_cp.wait()

    def col_copy(d):
        return pltpu.make_async_remote_copy(
            src_ref=colp, dst_ref=colp, send_sem=col_ssem.at[d], recv_sem=col_rsem,
            device_id={"pcol": lax.rem(me_q + d, nq)}, device_id_type=MESH)

    def row_copy(i, d):
        return pltpu.make_async_remote_copy(
            src_ref=rowp.at[i], dst_ref=rowp.at[i], send_sem=row_ssem.at[i, d], recv_sem=row_rsem.at[i],
            device_id={"prow": lax.rem(me_p + d, np_)}, device_id_type=MESH)

    @pl.when(me_q == 0)
    def _():
        @pl.loop(0, rs)
        def _(s):
            t = strip[pl.ds(s * LANES, LANES), :].T
            for c in range(NB + 1):
                colp[c, pl.ds(s, 1), :] = t[c:c + 1, :]
        for d in range(1, nq):
            col_copy(d).start()

    @pl.when(me_p == 0)
    def _():
        for s in range(cs):
            blk = arows[:, s * LANES:(s + 1) * LANES]
            for i in range(NB):
                rowp[i, s:s + 1, :] = blk[i:i + 1, :]
        for i in range(2):
            for d in range(1, np_):
                row_copy(i, d).start()

    for ref in (v_s, x_s, y_s, u_s):
        ref[...] = jnp.zeros(ref.shape, jnp.float32)

    @pl.when(me_q != 0)
    def _():
        col_copy(1).wait_recv()

    column_s[...] = colp[0]

    def y_copy(i, d, c):
        lo, n = (0, 8 + per) if c == 0 else (8 + c * per, per)
        ref = ybuf.at[i, me_p, pl.ds(lo, n), :]
        return pltpu.make_async_remote_copy(
            src_ref=ref, dst_ref=ref, send_sem=y_ssem.at[d, c], recv_sem=y_rsem.at[lax.rem(i, 2), d, c],
            device_id={"prow": lax.rem(me_p + d, np_)}, device_id_type=MESH)

    def x_copy(i, d, c):
        lo, n = (0, 8 + xper) if c == 0 else (8 + c * xper, xper)
        ref = xbuf.at[i, me_q, pl.ds(lo, n), :]
        return pltpu.make_async_remote_copy(
            src_ref=ref, dst_ref=ref, send_sem=x_ssem.at[d, c], recv_sem=x_rsem.at[lax.rem(i, 2), d, c],
            device_id={"pcol": lax.rem(me_q + d, nq)}, device_id_type=MESH)

    def scalar_tile(first, second, vec, unit):
        tile = jnp.zeros((8, LANES), jnp.float32)
        for k, (ref, w) in enumerate(((first, vec), (second, vec), (first, unit), (second, unit))):
            s = lane_sum(jnp.sum(ref[...] * w[None], axis=1))
            tile = jnp.where(lane8 == k, s, tile)
        s = jnp.where(sub8[:, :1] == 0, total(vec * unit), total(vec * vec))
        return jnp.where(lane8 == 4, s, tile)

    def unpack(tile):
        return [jnp.broadcast_to(lane_sum(jnp.where(lane8 == k, tile, 0.0)), (8, LANES)) for k in range(5)]

    def combine(coef_a, ref_a, coef_b, ref_b):
        acc = coef_a[0:1] * ref_a[0] + coef_b[0:1] * ref_b[0]
        for j in range(1, NB):
            acc = acc + (coef_a[j:j + 1] * ref_a[j] + coef_b[j:j + 1] * ref_b[j])
        return acc

    @pl.loop(0, NB)
    def _(i):
        masked = jnp.where(row_gl >= i, column_s[...], 0.0)
        unit_r = (row_gl == i).astype(jnp.float32)
        column_s[...] = masked

        @pl.loop(0, rs, unroll=min(8, rs))
        def _(s):
            row = jnp.broadcast_to(column_s[pl.ds(s, 1), :], (8, LANES))
            for g in range(LANES // 8):
                col = lane_sum(jnp.where(lane8 == sub8 + 8 * g, row, 0.0))
                vb[pl.ds(s * LANES + 8 * g, 8), :] = jnp.broadcast_to(col, (8, LANES))

        ybuf[i, me_p, 0:8, :] = scalar_tile(v_s, x_s, masked, unit_r)
        for c in range(YC):
            @pl.when(i == 0)
            def _(c=c):
                a_cps[c].wait()

            def body(g, accs):
                accs = list(accs)
                for k in range(8):
                    r = pl.ds(pl.multiple_of(g * 64 + 8 * k, 8), 8)
                    v = vb[r, :]
                    for j in range(per):
                        lo = c * chunk + j * LANES
                        m = (k % 2) * per + j
                        accs[m] = accs[m] + v * a[r, lo:lo + LANES]
                return tuple(accs)

            accs = lax.fori_loop(0, rows // 64, body, (jnp.zeros((8, LANES), jnp.float32),) * (2 * per))
            for j in range(per):
                t = 8 + c * per + j
                ybuf[i, me_p, t:t + 1, :] = jnp.sum(accs[j] + accs[per + j], axis=0, keepdims=True)
            for d in range(1, np_):
                y_copy(i, d, c).start()

        @pl.when(jnp.logical_and(me_p == 0, i < NB - 2))
        def _():
            for d in range(1, np_):
                row_copy(i + 2, d).start()

        @pl.when(me_p != 0)
        def _():
            row_copy(i, 1).wait_recv()

        for c in range(YC):
            for d in range(1, np_):
                y_copy(i, d, c).wait()
        summed = ybuf[i, 0]
        for p in range(1, np_):
            summed = summed + ybuf[i, p]
        v_coef, x_coef, v_at, x_at, misc = unpack(summed[0:8])
        beta, tau, denom = householder(misc[0:1], misc[1:2])
        row_eff = rowp[i] - combine(v_at, y_s, x_at, u_s)
        inv = 1.0 / denom
        trans = (summed[8:] - combine(v_coef, y_s, x_coef, u_s) - beta * row_eff) * inv
        y_new = jnp.where(col_gl > i, tau * trans, 0.0)
        v_s[i] = (masked - beta * unit_r) * inv
        y_s[i] = y_new
        scal_o[0, pl.ds(i, 1), :] = beta
        scal_o[2, pl.ds(i, 1), :] = tau

        row_m = jnp.where(col_gl > i, row_eff - y_new, 0.0)
        unit_c = (col_gl == i + 1).astype(jnp.float32)
        ub[...] = row_m
        xbuf[i, me_q, 0:8, :] = scalar_tile(y_s, u_s, row_m, unit_c)
        for c in range(XC):
            @pl.loop(c * xper, (c + 1) * xper, unroll=min(4, xper))
            def _(s):
                us = [jnp.broadcast_to(ub[j:j + 1, :], (8, LANES)) for j in range(cs)]
                tile = jnp.zeros((8, LANES), jnp.float32)
                for g in range(LANES // 8):
                    r = pl.ds(pl.multiple_of(s * LANES + 8 * g, 8), 8)
                    p0 = us[0] * a[r, 0:LANES]
                    p1 = us[1] * a[r, LANES:2 * LANES]
                    for j in range(2, cs, 2):
                        p0 = p0 + us[j] * a[r, j * LANES:(j + 1) * LANES]
                        p1 = p1 + us[j + 1] * a[r, (j + 1) * LANES:(j + 2) * LANES]
                    tile = jnp.where(lane8 == sub8 + 8 * g, lane_sum(p0 + p1), tile)
                xbuf[i, me_q, pl.ds(8 + s, 1), :] = jnp.sum(tile, axis=0, keepdims=True)
            for d in range(1, nq):
                x_copy(i, d, c).start()
        for c in range(XC):
            for d in range(1, nq):
                x_copy(i, d, c).wait()
        xsum = xbuf[i, 0]
        for q in range(1, nq):
            xsum = xsum + xbuf[i, q]
        y_coef, u_coef, y_at, u_at, misc2 = unpack(xsum[0:8])
        beta2, tau2, denom2 = householder(misc2[0:1], misc2[1:2])
        col_next = colp[i + 1] - combine(y_at, v_s, u_at, x_s)
        inv2 = 1.0 / denom2
        prod = (xsum[8:] - combine(y_coef, v_s, u_coef, x_s) - beta2 * col_next) * inv2
        x_new = jnp.where(row_gl > i, tau2 * prod, 0.0)
        x_s[i] = x_new
        u_s[i] = (row_m - beta2 * unit_c) * inv2
        scal_o[1, pl.ds(i, 1), :] = beta2
        scal_o[3, pl.ds(i, 1), :] = tau2
        column_s[...] = col_next - x_new

    for s in range(rs):
        left_o[0:NB, s * LANES:(s + 1) * LANES] = v_s[:, s, :]
        left_o[NB:, s * LANES:(s + 1) * LANES] = x_s[:, s, :]
    for s in range(cs):
        right_o[0:NB, s * LANES:(s + 1) * LANES] = y_s[:, s, :]
        right_o[NB:, s * LANES:(s + 1) * LANES] = u_s[:, s, :]

    @pl.when(me_q == 0)
    def _():
        for d in range(1, nq):
            col_copy(d).wait_send()

    @pl.when(me_p == 0)
    def _():
        @pl.loop(0, NB)
        def _(i):
            for d in range(1, np_):
                row_copy(i, d).wait_send()


def reduce_panel(matrix, np_, nq):
    rows, cols = matrix.shape
    rs, cs = rows // LANES, cols // LANES
    f32 = jnp.float32
    vmem = pl.BlockSpec(memory_space=pltpu.VMEM)
    dma = pltpu.SemaphoreType.DMA
    return pl.pallas_call(
        functools.partial(panel_kernel, np_, nq),
        out_shape=(jax.ShapeDtypeStruct((2 * NB, rows), f32),
                   jax.ShapeDtypeStruct((2 * NB, cols), f32),
                   jax.ShapeDtypeStruct((4, NB, LANES), f32)),
        in_specs=[pl.BlockSpec(memory_space=pl.ANY)],
        out_specs=(vmem, vmem, vmem),
        scratch_shapes=[
            pltpu.VMEM((rows, cols), f32),
            pltpu.VMEM((rows, LANES), f32),
            pltpu.VMEM((NB, cols), f32),
            pltpu.VMEM((NB + 1, rs, LANES), f32),
            pltpu.VMEM((NB, cs, LANES), f32),
            pltpu.VMEM((NB, rs, LANES), f32),
            pltpu.VMEM((NB, rs, LANES), f32),
            pltpu.VMEM((NB, cs, LANES), f32),
            pltpu.VMEM((NB, cs, LANES), f32),
            pltpu.VMEM((rows, LANES), f32),
            pltpu.VMEM((cs, LANES), f32),
            pltpu.VMEM((NB, np_, 8 + cs, LANES), f32),
            pltpu.VMEM((NB, nq, 8 + rs, LANES), f32),
            pltpu.VMEM((rs, LANES), f32),
            dma((YC,)), dma, dma,
            dma((nq,)), dma, dma((NB, np_)), dma((NB,)),
            dma((np_, YC)), dma((2, np_, YC)), dma((nq, XC)), dma((2, nq, XC)),
        ],
        compiler_params=pltpu.CompilerParams(
            collective_id=0, has_side_effects=True, vmem_limit_bytes=60 * 1024 * 1024),
    )(matrix)


def pieces(x):
    hi = x.astype(jnp.bfloat16)
    rest = x - hi.astype(jnp.float32)
    mid = rest.astype(jnp.bfloat16)
    lo = (rest - mid.astype(jnp.float32)).astype(jnp.bfloat16)
    return hi, mid, lo


def update_kernel(a_ref, left_ref, right_ref, scal_ref, out_ref):
    me_p = lax.axis_index("prow")
    me_q = lax.axis_index("pcol")
    step = pl.program_id(0)
    block, cols = a_ref.shape
    lh, lm, ll = pieces(left_ref[...])
    rh, rm, rl = pieces(right_ref[...])
    left = jnp.concatenate([lh, lh, lh, lm, lm, ll], axis=0)
    right = jnp.concatenate([rh, rm, rl, rh, rm, rh], axis=0)
    dims = (((0,), (0,)), ((), ()))
    out_ref[...] = a_ref[...] - lax.dot_general(left, right, dims, preferred_element_type=jnp.float32)

    k = left.shape[0]
    src = lax.broadcasted_iota(jnp.int32, (k, LANES), 0)
    lane = lax.broadcasted_iota(jnp.int32, (k, LANES), 1)
    pick = jnp.logical_and(
        lane < NB, (src == lane) | (src == lane + 6 * NB) | (src == lane + 10 * NB))
    vt = lax.dot_general(left, jnp.where(pick, 1.0, 0.0).astype(jnp.bfloat16), dims,
                         preferred_element_type=jnp.float32)

    @pl.when(me_q == 0)
    def _():
        lanes = lax.broadcasted_iota(jnp.int32, (block, LANES), 1)
        out_ref[:, 0:LANES] = jnp.where(lanes < NB, vt, out_ref[:, 0:LANES])

    @pl.when(jnp.logical_and(me_p == 0, step == 0))
    def _():
        out_ref[0:NB, :] = right_ref[NB:, :]

        @pl.when(me_q == 0)
        def _():
            r = lax.broadcasted_iota(jnp.int32, (NB, LANES), 0)
            c = lax.broadcasted_iota(jnp.int32, (NB, LANES), 1)
            out_ref[0:NB, 0:LANES] = jnp.where(
                c < r, vt[0:NB, :],
                jnp.where(c == r, scal_ref[0], jnp.where(c == r + 1, scal_ref[1], right_ref[NB:, 0:LANES])))


def apply_panel(matrix, left, right, scal):
    rows, cols = matrix.shape
    block = min(rows, 256)
    return pl.pallas_call(
        update_kernel,
        out_shape=jax.ShapeDtypeStruct((rows, cols), jnp.float32),
        grid=(rows // block,),
        in_specs=[
            pl.BlockSpec((block, cols), lambda i: (i, 0)),
            pl.BlockSpec((2 * NB, block), lambda i: (0, i)),
            pl.BlockSpec((2 * NB, cols), lambda i: (0, 0)),
            pl.BlockSpec((4, NB, LANES), lambda i: (0, 0, 0)),
        ],
        out_specs=pl.BlockSpec((block, cols), lambda i: (i, 0)),
        compiler_params=pltpu.CompilerParams(vmem_limit_bytes=48 * 1024 * 1024),
    )(matrix, left, right, scal)


def solution(mesh):
    np_, nq = mesh.shape["prow"], mesh.shape["pcol"]

    def per_device(matrix):
        left, right, scal = reduce_panel(matrix, np_, nq)
        return apply_panel(matrix, left, right, scal), scal[2:4, :, 0]

    return jax.shard_map(
        per_device, mesh=mesh, in_specs=(P("prow", "pcol"),),
        out_specs=(P("prow", "pcol"), P()), check_vma=False)
```
